32 devices in a mesh: nodes: 2 (over core), gx: 4 (over z), gy: 4 (over y, x).
Axes of the slice: x: 2, y: 2, z: 4, core: 2. Of those that a mesh axis runs over, the one named last changes fastest.
Arguments:
- field_modes: float32 [4, 9, 256, 512], P(None, None, 'gx', 'gy'), may hold values from -4 to 4, as said below
- node_points: float32 [768, 8], replicated, may hold values from -1 to 1
- quad_weight: float32 [768], replicated, may hold values from 0.5 to 2
- group_of: int32 [768], replicated, may hold values from 0 to 2, as said below
Outputs:
- mean_field: float32 [256, 512], P('gx', 'gy')
- variance_field: float32 [256, 512], P('gx', 'gy')
The draws below stay inside these ranges and needn't reach their ends.
Inputs may be any that keep to these rules, and one draw needn't show every extreme that they name: `group_of`: one of the two groups (which one varies) is given exactly 384 nodes, the other between 48 and 96; all other nodes hold 2. `field_modes`: diffusivity fields (index 3) give a diffusivity between 0.1 and 1.4 at every node point in range; the other fields lie within the range.
All inputs are finite; a program needn't handle non-finite values.
Results may differ from the reference program's by a relative error of at most 0.00021.
Values sent between devices are 32-bit elements; how exact they have to be, the bound alone decides.
No kernel may reach another device: no remote copies, remote signals or barrier semaphores. Data moves between devices by JAX's collectives and lax.ppermute only.
A program may use at most 192 MiB of HBM per device.

```python
import math
import jax
import jax.numpy as jnp
from jax import lax

BUSY = 384
STEPS = 4
DIMS = 8
NODES = 768
NX = 256
NY = 512


def draw_group_of(key, part):
    key_busy = jax.random.fold_in(key, 11)
    key_light = jax.random.fold_in(key, 12)
    key_order = jax.random.fold_in(key, 13)
    busy_group = jax.random.randint(key_busy, (), 0, 2)
    light_count = jax.random.randint(key_light, (), BUSY // 8, BUSY // 4 + 1)
    ordering = jax.random.permutation(key_order, NODES)
    placed = jnp.argsort(ordering)
    labels = jnp.where(placed < BUSY, busy_group, jnp.where(placed < BUSY + light_count, 1 - busy_group, 2))
    return labels.astype(jnp.int32)


def draw_field_modes(key, part):
    keys = [jax.random.fold_in(key, 21 + number) for number in range(5)]
    shaped = (DIMS + 1, NX, NY)
    initial = jnp.clip(jax.random.normal(keys[0], shaped), -4.0, 4.0)
    speeds = jnp.clip(0.25 * jax.random.normal(keys[1], (2,) + shaped), -1.0, 1.0)
    diff_base = jax.random.uniform(keys[2], (1, NX, NY), minval=0.5, maxval=1.0)
    diff_modes = jax.random.uniform(keys[4], (DIMS, NX, NY), minval=-0.05, maxval=0.05)
    diffusion = jnp.concatenate([diff_base, diff_modes], axis=0)
    return jnp.stack([initial, speeds[0], speeds[1], diffusion]).astype(jnp.float32)


def setup_inputs(seed: int = 0) -> dict:
    splits = jax.random.split(jax.random.key(seed), 5)
    return {
        "field_modes": draw_field_modes(jax.random.fold_in(splits[4], 71), 0),
        "node_points": jnp.clip(jax.random.uniform(splits[1], (NODES, DIMS), jnp.float32, -1.0, 1.0), -1.0, 1.0),
        "quad_weight": jnp.clip(jnp.exp(jax.random.uniform(splits[2], (NODES,), jnp.float32, math.log(0.5), math.log(2.0))), 0.5, 2.0),
        "group_of": draw_group_of(jax.random.fold_in(splits[4], 71), 0),
    }


TIME_STEP = 0.15


def advance_cells(centre, east_side, west_side, north_side, south_side, x_speed, y_speed, diffusion):
    laplace = (east_side + west_side + north_side + south_side) - 4.0 * centre
    transport = x_speed * ((east_side - west_side) * 0.5) + y_speed * ((north_side - south_side) * 0.5)
    return centre + TIME_STEP * (diffusion * laplace - transport)


def evolve(coefficients, field_modes):
    params = jnp.einsum("bk,ckxy->bcxy", coefficients, field_modes, precision=lax.Precision.HIGHEST)
    state = params[:, 0]
    for section in range(STEPS):
        east_side = jnp.roll(state, -1, axis=1)
        west_side = jnp.roll(state, 1, axis=1)
        north_side = jnp.roll(state, -1, axis=2)
        south_side = jnp.roll(state, 1, axis=2)
        state = advance_cells(state, east_side, west_side, north_side, south_side, params[:, 1], params[:, 2], params[:, 3])
    return state


def reference(field_modes, node_points, quad_weight, group_of):
    included = (group_of < 2).astype(jnp.float32)
    weight = quad_weight * included
    weight_total = jnp.sum(weight)
    coefficients = jnp.concatenate([jnp.ones((NODES, 1), jnp.float32), node_points], axis=1)
    blocks = NODES // 16
    coeff_blocks = coefficients.reshape(blocks, 16, DIMS + 1)
    weight_blocks = weight.reshape(blocks, 16)

    def accumulate(carry, pieces):
        state = evolve(pieces[0], field_modes)
        first = carry[0] + jnp.einsum("b,bxy->xy", pieces[1], state, precision=lax.Precision.HIGHEST)
        second = carry[1] + jnp.einsum("b,bxy->xy", pieces[1], state * state, precision=lax.Precision.HIGHEST)
        return (first, second), None

    start = (jnp.zeros((NX, NY), jnp.float32), jnp.zeros((NX, NY), jnp.float32))
    (first, second), unused = lax.scan(accumulate, start, (coeff_blocks, weight_blocks))
    mean_field = first / weight_total
    variance_field = second / weight_total - mean_field * mean_field
    return mean_field, variance_field
```

```python
import jax
import jax.numpy as jnp
from jax import lax
from jax.experimental import pallas as pl
from jax.experimental.pallas import tpu as pltpu
from jax.sharding import PartitionSpec as P

STEPS = 4
TIME_STEP = 0.15
LANES = 128
SUBLANES = 8
BLOCK = 4


def split(x):
    high = x.astype(jnp.bfloat16).astype(jnp.float32)
    return high, x - high


def moments_kernel(centre_ref, edge_ref, table_ref, weight_ref, order_ref, out_ref, w_ref, coef_ref, state_ref):
    trips = centre_ref.shape[0] // BLOCK
    cells = order_ref.shape[0]
    slots = table_ref.shape[2]
    kinds = table_ref.shape[0]
    groups = slots // LANES
    out_ref[...] = jnp.zeros_like(out_ref)
    for kind in range(kinds):
        high, low = split(table_ref[kind])
        w_ref[kind] = jnp.concatenate([high, high, low], axis=0).astype(jnp.bfloat16)

    def body(trip, carry):
        def slot(row):
            lag = row // BLOCK
            return ((trip + lag) & 1) * BLOCK + (row - lag * BLOCK)

        lhs = []
        for row in range(BLOCK):
            index = trip * BLOCK + row
            field = jnp.concatenate([centre_ref[index], edge_ref[index]], axis=1)
            high, low = split(field)
            stacked = jnp.concatenate([high, low, high], axis=0).astype(jnp.bfloat16)
            lhs.append(
                lax.dot_general(
                    order_ref[...], stacked, (((1,), (1,)), ((), ())), preferred_element_type=jnp.float32
                )
            )
        lhs = jnp.concatenate(lhs, axis=0).astype(jnp.bfloat16)
        for kind in range(kinds):
            values = jnp.dot(lhs, w_ref[kind], preferred_element_type=jnp.float32)
            for row in range(BLOCK):
                part = values[row * cells : (row + 1) * cells]
                if kind == 0:
                    state_ref[0, slot(row)] = part
                else:
                    coef_ref[kind - 1, slot(row)] = part

        firsts, seconds = [], []
        for step in range(1, STEPS + 1):
            for offset in range(BLOCK):
                row = offset - step
                first = second = None
                for group in range(groups):
                    lanes = pl.ds(group * LANES, LANES)
                    centre = state_ref[step - 1, slot(row), :, lanes]
                    west = state_ref[step - 1, slot(row - 1), :, lanes]
                    east = state_ref[step - 1, slot(row + 1), :, lanes]
                    wrap_north = pltpu.roll(centre[:SUBLANES], SUBLANES - 1, 0)
                    wrap_south = pltpu.roll(centre[cells - SUBLANES :], 1, 0)
                    north = jnp.concatenate([centre[SUBLANES:], wrap_north], axis=0)
                    south = jnp.concatenate([wrap_south, centre[: cells - SUBLANES]], axis=0)
                    c0, ce, cw, cn, cs = (coef_ref[k, slot(row), :, lanes] for k in range(5))
                    new = (c0 * centre + (ce * east + cw * west)) + (cn * north + cs * south)
                    if step < STEPS:
                        state_ref[step, slot(row), :, lanes] = new
                    else:
                        scaled = new * weight_ref[:, lanes]
                        squared = scaled * new
                        first = scaled if first is None else first + scaled
                        second = squared if second is None else second + squared
                if step == STEPS:
                    firsts.append(first)
                    seconds.append(second)

        @pl.when(trip * BLOCK >= 2 * STEPS)
        def _():
            column = lax.broadcasted_iota(jnp.int32, (cells, out_ref.shape[2]), 1)
            base = trip * BLOCK - 2 * STEPS
            for which, sums in enumerate((firsts, seconds)):
                kept = out_ref[which]
                for offset in range(BLOCK):
                    total = jnp.sum(sums[offset], axis=1, keepdims=True)
                    kept = jnp.where(column == base + offset, total, kept)
                out_ref[which] = kept

        return carry

    lax.fori_loop(0, trips, body, 0)


def on_device(field_modes, node_points, quad_weight, group_of):
    kinds, modes, tile_rows, tile_cols = field_modes.shape
    node_count = group_of.shape[0]
    members = lax.axis_size("nodes")
    most = node_count // 2 + node_count // 8
    slots = -(-most // (members * LANES)) * LANES
    member = lax.axis_index("nodes")

    included = group_of < 2
    weight = quad_weight * included.astype(jnp.float32)
    number = jnp.arange(node_count, dtype=jnp.int32)
    before = (number[None, :] < number[:, None]) & included[None, :]
    position = jnp.sum(before.astype(jnp.float32), axis=1).astype(jnp.int32)
    target = jnp.arange(slots, dtype=jnp.int32) * members + member
    select = (included[:, None] & (position[:, None] == target[None, :])).astype(jnp.float32)
    columns = jnp.concatenate([jnp.ones((node_count, 1), jnp.float32), node_points, quad_weight[:, None]], axis=1)
    chosen = lax.dot_general(columns, select, (((0,), (0,)), ((), ())), precision=lax.Precision.HIGHEST)
    slot_coeff, slot_weight = chosen[: modes], chosen[modes:]
    half = 0.5 * TIME_STEP
    mix = (
        ((1.0, 0.0, 0.0, 0.0), 0.0),
        ((0.0, 0.0, 0.0, -4.0 * TIME_STEP), 1.0),
        ((0.0, -half, 0.0, TIME_STEP), 0.0),
        ((0.0, half, 0.0, TIME_STEP), 0.0),
        ((0.0, 0.0, -half, TIME_STEP), 0.0),
        ((0.0, 0.0, half, TIME_STEP), 0.0),
    )
    used = kinds * modes
    padded = -(-(used + 1) // SUBLANES) * SUBLANES
    mixes = jnp.array([m for m, _ in mix], jnp.float32)
    constant = jnp.array([c for _, c in mix], jnp.float32)
    table = (mixes[:, :, None, None] * slot_coeff[None, None]).reshape(len(mix), used, slots)
    table = jnp.concatenate(
        [
            table,
            jnp.broadcast_to(constant[:, None, None], (len(mix), 1, slots)),
            jnp.zeros((len(mix), padded - used - 1, slots), jnp.float32),
        ],
        axis=1,
    )

    def ring(axis):
        size = lax.axis_size(axis)
        up = [(i, (i + 1) % size) for i in range(size)]
        return up, [(j, i) for i, j in up]

    fields = field_modes.reshape(used, tile_rows, tile_cols)
    up, down = ring("gx")
    above = lax.ppermute(fields[:, tile_rows - STEPS :], "gx", up)
    below = lax.ppermute(fields[:, :STEPS], "gx", down)
    tall = jnp.concatenate([above, fields, below], axis=1)
    up, down = ring("gy")
    left = lax.ppermute(jnp.transpose(tall[:, :, tile_cols - STEPS :], (2, 0, 1)), "gy", up)
    right = lax.ppermute(jnp.transpose(tall[:, :, :STEPS], (2, 0, 1)), "gy", down)
    edge = jnp.transpose(jnp.concatenate([left, right], axis=0), (2, 1, 0))
    centre = jnp.transpose(tall, (1, 0, 2))
    fill = ((0, 0), (0, padded - used), (0, 0))
    centre = jnp.pad(centre, fill, constant_values=1.0)
    edge = jnp.pad(edge, fill, constant_values=1.0)

    cells = tile_cols + 2 * STEPS
    per = cells // SUBLANES
    place = jnp.arange(cells, dtype=jnp.int32)
    wanted = (place % SUBLANES) * per + place // SUBLANES - STEPS
    source = jnp.where(
        wanted < 0, tile_cols + STEPS + wanted, jnp.where(wanted < tile_cols, wanted, wanted + STEPS)
    )
    order = (source[:, None] == place[None, :]).astype(jnp.bfloat16)

    sums = pl.pallas_call(
        moments_kernel,
        out_shape=jax.ShapeDtypeStruct((2, cells, tile_rows), jnp.float32),
        scratch_shapes=[
            pltpu.VMEM((len(mix), 3 * padded, slots), jnp.bfloat16),
            pltpu.VMEM((5, 2 * BLOCK, cells, slots), jnp.float32),
            pltpu.VMEM((STEPS, 2 * BLOCK, cells, slots), jnp.float32),
        ],
        compiler_params=pltpu.CompilerParams(vmem_limit_bytes=48 * 1024 * 1024),
        name="moments",
    )(centre, edge, table, slot_weight, order)

    total = sums
    for shift in range(1, members):
        ring_pairs = [(i, (i + shift) % members) for i in range(members)]
        total = total + lax.ppermute(sums, "nodes", ring_pairs)
    weight_total = jnp.sum(weight)
    mean = total[0] / weight_total
    variance = total[1] / weight_total - mean * mean
    fields_out = jnp.stack([mean, variance]).reshape(2, per, SUBLANES, tile_rows)
    fields_out = jnp.transpose(fields_out, (0, 3, 2, 1)).reshape(2, tile_rows, cells)
    fields_out = fields_out[:, :, STEPS : STEPS + tile_cols]
    return fields_out[0], fields_out[1]


def solution(mesh):
    placed = (P(None, None, "gx", "gy"), P(), P(), P())
    return jax.shard_map(
        on_device,
        mesh=mesh,
        in_specs=placed,
        out_specs=(P("gx", "gy"), P("gx", "gy")),
        check_vma=False,
    )
```

```python
import jax
import jax.numpy as jnp
from jax import lax
from jax.experimental import pallas as pl
from jax.experimental.pallas import tpu as pltpu
from jax.sharding import PartitionSpec as P

STEPS = 4
TIME_STEP = 0.15
LANES = 128
SUBLANES = 8
BLOCK = 2
UNROLL = 4
RING = BLOCK * UNROLL


def split(x):
    high = x.astype(jnp.bfloat16).astype(jnp.float32)
    return high, x - high


def moments_kernel(centre_ref, edge_ref, table_ref, weight_ref, order_ref, out_ref, w_ref, lhs_ref, *rings):
    rows = centre_ref.shape[0]
    cells = order_ref.shape[0]
    slots = table_ref.shape[2]
    kinds = table_ref.shape[0]
    groups = slots // LANES
    per = cells // SUBLANES
    states = (rings[0],) + rings[kinds:]
    coefs = rings[1:kinds]
    out_ref[...] = jnp.zeros_like(out_ref)
    for kind in range(kinds):
        high, low = split(table_ref[kind])
        w_ref[kind] = jnp.concatenate([high, high, low], axis=0).astype(jnp.bfloat16)
    column = lax.broadcasted_iota(jnp.int32, (SUBLANES, out_ref.shape[2]), 1)

    def left_side(base, half):
        parts = []
        for row in range(BLOCK):
            index = jnp.minimum(base + row, rows - 1)
            field = jnp.concatenate([centre_ref[index], edge_ref[index]], axis=1)
            high, low = split(field)
            stacked = jnp.concatenate([high, low, high], axis=0).astype(jnp.bfloat16)
            parts.append(
                lax.dot_general(
                    order_ref[...], stacked, (((1,), (1,)), ((), ())), preferred_element_type=jnp.float32
                )
            )
        lhs_ref[half] = jnp.concatenate(parts, axis=0).astype(jnp.bfloat16)

    def parameter(kind, half):
        values = jnp.dot(lhs_ref[half], w_ref[kind], preferred_element_type=jnp.float32)
        for row in range(BLOCK):
            rings[kind][half * BLOCK + row] = values[row * cells : (row + 1) * cells]

    def tile(ref, row, part, group):
        return ref[row % RING, part * SUBLANES : (part + 1) * SUBLANES, group * LANES : (group + 1) * LANES]

    def advance(step, row, base):
        source = states[step - 1]
        weights = [
            jnp.broadcast_to(weight_ref[:, g * LANES : (g + 1) * LANES], (SUBLANES, LANES)) for g in range(groups)
        ]
        start = [tile(source, row, 0, g) for g in range(groups)]
        last = [tile(source, row, per - 1, g) for g in range(groups)]
        south = [pltpu.roll(x, 1, 0) for x in last]
        wrapped = [pltpu.roll(x, SUBLANES - 1, 0) for x in start]
        centre = start
        for part in range(per):
            first = second = None
            north = wrapped if part == per - 1 else [tile(source, row, part + 1, g) for g in range(groups)]
            for g in range(groups):
                west = tile(source, row - 1, part, g)
                east = tile(source, row + 1, part, g)
                c0, ce, cw, cn, cs = (tile(ref, row, part, g) for ref in coefs)
                fresh = (c0 * centre[g] + (ce * east + cw * west)) + (cn * north[g] + cs * south[g])
                if step < STEPS:
                    states[step][
                        row % RING, part * SUBLANES : (part + 1) * SUBLANES, g * LANES : (g + 1) * LANES
                    ] = fresh
                else:
                    scaled = fresh * weights[g]
                    squared = scaled * fresh
                    first = scaled if first is None else first + scaled
                    second = squared if second is None else second + squared
            south, centre = centre, north
            if step == STEPS:
                here = column == base + row - STEPS
                rows_here = slice(part * SUBLANES, (part + 1) * SUBLANES)
                for which, sums in enumerate((first, second)):
                    total = jnp.sum(sums, axis=1, keepdims=True)
                    out_ref[which, rows_here] = jnp.where(here, total, out_ref[which, rows_here])

    left_side(0, 0)
    for kind in range(kinds):
        parameter(kind, 0)

    def body(trip, carry):
        base = trip * RING
        for half in range(UNROLL):
            following = (half + 1) % UNROLL
            left_side(base + (half + 1) * BLOCK, following)
            kind = 0
            units = [(s, half * BLOCK + o - s) for s in range(1, STEPS + 1) for o in range(BLOCK)]
            for number, (step, row) in enumerate(units):
                advance(step, row, base)
                while kind * len(units) < kinds * (number + 1):
                    parameter(kind, following)
                    kind += 1
        return carry

    lax.fori_loop(0, pl.cdiv(rows, RING), body, 0)


def on_device(field_modes, node_points, quad_weight, group_of):
    kinds, modes, tile_rows, tile_cols = field_modes.shape
    node_count = group_of.shape[0]
    members = lax.axis_size("nodes")
    most = node_count // 2 + node_count // 8
    slots = -(-most // (members * LANES)) * LANES
    member = lax.axis_index("nodes")

    included = group_of < 2
    weight = quad_weight * included.astype(jnp.float32)
    number = jnp.arange(node_count, dtype=jnp.int32)
    before = (number[None, :] < number[:, None]) & included[None, :]
    position = jnp.sum(before.astype(jnp.float32), axis=1).astype(jnp.int32)
    target = jnp.arange(slots, dtype=jnp.int32) * members + member
    select = (included[:, None] & (position[:, None] == target[None, :])).astype(jnp.float32)
    columns = jnp.concatenate([jnp.ones((node_count, 1), jnp.float32), node_points, quad_weight[:, None]], axis=1)
    chosen = lax.dot_general(columns, select, (((0,), (0,)), ((), ())), precision=lax.Precision.HIGHEST)
    slot_coeff, slot_weight = chosen[: modes], chosen[modes:]
    half = 0.5 * TIME_STEP
    mix = (
        ((1.0, 0.0, 0.0, 0.0), 0.0),
        ((0.0, 0.0, 0.0, -4.0 * TIME_STEP), 1.0),
        ((0.0, -half, 0.0, TIME_STEP), 0.0),
        ((0.0, half, 0.0, TIME_STEP), 0.0),
        ((0.0, 0.0, -half, TIME_STEP), 0.0),
        ((0.0, 0.0, half, TIME_STEP), 0.0),
    )
    used = kinds * modes
    padded = -(-(used + 1) // SUBLANES) * SUBLANES
    mixes = jnp.array([m for m, _ in mix], jnp.float32)
    constant = jnp.array([c for _, c in mix], jnp.float32)
    table = (mixes[:, :, None, None] * slot_coeff[None, None]).reshape(len(mix), used, slots)
    table = jnp.concatenate(
        [
            table,
            jnp.broadcast_to(constant[:, None, None], (len(mix), 1, slots)),
            jnp.zeros((len(mix), padded - used - 1, slots), jnp.float32),
        ],
        axis=1,
    )

    def ring(axis):
        size = lax.axis_size(axis)
        up = [(i, (i + 1) % size) for i in range(size)]
        return up, [(j, i) for i, j in up]

    fields = field_modes.reshape(used, tile_rows, tile_cols)
    up, down = ring("gx")
    above = lax.ppermute(fields[:, tile_rows - STEPS :], "gx", up)
    below = lax.ppermute(fields[:, :STEPS], "gx", down)
    tall = jnp.concatenate([above, fields, below], axis=1)
    up, down = ring("gy")
    left = lax.ppermute(jnp.transpose(tall[:, :, tile_cols - STEPS :], (2, 0, 1)), "gy", up)
    right = lax.ppermute(jnp.transpose(tall[:, :, :STEPS], (2, 0, 1)), "gy", down)
    edge = jnp.transpose(jnp.concatenate([left, right], axis=0), (2, 1, 0))
    centre = jnp.transpose(tall, (1, 0, 2))
    fill = ((0, 0), (0, padded - used), (0, 0))
    centre = jnp.pad(centre, fill, constant_values=1.0)
    edge = jnp.pad(edge, fill, constant_values=1.0)

    cells = tile_cols + 2 * STEPS
    per = cells // SUBLANES
    place = jnp.arange(cells, dtype=jnp.int32)
    wanted = (place % SUBLANES) * per + place // SUBLANES - STEPS
    source = jnp.where(
        wanted < 0, tile_cols + STEPS + wanted, jnp.where(wanted < tile_cols, wanted, wanted + STEPS)
    )
    order = (source[:, None] == place[None, :]).astype(jnp.bfloat16)

    sums = pl.pallas_call(
        moments_kernel,
        out_shape=jax.ShapeDtypeStruct((2, cells, tile_rows), jnp.float32),
        scratch_shapes=[
            pltpu.VMEM((len(mix), 3 * padded, slots), jnp.bfloat16),
            pltpu.VMEM((UNROLL, BLOCK * cells, 3 * padded), jnp.bfloat16),
        ]
        + [pltpu.VMEM((RING, cells, slots), jnp.float32)] * (len(mix) + STEPS - 1),
        compiler_params=pltpu.CompilerParams(vmem_limit_bytes=48 * 1024 * 1024),
        name="moments",
    )(centre, edge, table, slot_weight, order)

    total = sums
    for shift in range(1, members):
        ring_pairs = [(i, (i + shift) % members) for i in range(members)]
        total = total + lax.ppermute(sums, "nodes", ring_pairs)
    weight_total = jnp.sum(weight)
    mean = total[0] / weight_total
    variance = total[1] / weight_total - mean * mean
    fields_out = jnp.stack([mean, variance]).reshape(2, per, SUBLANES, tile_rows)
    fields_out = jnp.transpose(fields_out, (0, 3, 2, 1)).reshape(2, tile_rows, cells)
    fields_out = fields_out[:, :, STEPS : STEPS + tile_cols]
    return fields_out[0], fields_out[1]


def solution(mesh):
    placed = (P(None, None, "gx", "gy"), P(), P(), P())
    return jax.shard_map(
        on_device,
        mesh=mesh,
        in_specs=placed,
        out_specs=(P("gx", "gy"), P("gx", "gy")),
        check_vma=False,
    )
```

```python
import jax
import jax.numpy as jnp
from jax import lax
from jax.experimental import pallas as pl
from jax.experimental.pallas import tpu as pltpu
from jax.sharding import PartitionSpec as P

STEPS = 4
TIME_STEP = 0.15
LANES = 128
SUBLANES = 8
BLOCK = 2
UNROLL = 4
RING = BLOCK * UNROLL


def split(x):
    high = x.astype(jnp.bfloat16).astype(jnp.float32)
    return high, x - high


def moments_kernel(centre_ref, edge_ref, table_ref, weight_ref, order_ref, out_ref, w_ref, lhs_ref, *rings):
    rows = centre_ref.shape[0]
    cells = order_ref.shape[0]
    slots = table_ref.shape[2]
    kinds = table_ref.shape[0]
    groups = slots // LANES
    per = cells // SUBLANES
    states = (rings[0],) + rings[kinds:]
    coefs = rings[1:kinds]
    out_ref[...] = jnp.zeros_like(out_ref)
    for kind in range(kinds):
        high, low = split(table_ref[kind])
        w_ref[kind] = jnp.concatenate([high, high, low], axis=0).astype(jnp.bfloat16)
    column = lax.broadcasted_iota(jnp.int32, (SUBLANES, out_ref.shape[2]), 1)

    def left_side(base, half):
        parts = []
        for row in range(BLOCK):
            index = jnp.minimum(base + row, rows - 1)
            field = jnp.concatenate([centre_ref[index], edge_ref[index]], axis=1)
            high, low = split(field)
            stacked = jnp.concatenate([high, low, high], axis=0).astype(jnp.bfloat16)
            parts.append(
                lax.dot_general(
                    order_ref[...], stacked, (((1,), (1,)), ((), ())), preferred_element_type=jnp.float32
                )
            )
        lhs_ref[half] = jnp.concatenate(parts, axis=0).astype(jnp.bfloat16)

    def parameter(kind, half):
        values = jnp.dot(lhs_ref[half], w_ref[kind], preferred_element_type=jnp.float32)
        for row in range(BLOCK):
            rings[kind][half * BLOCK + row] = values[row * cells : (row + 1) * cells]

    def tile(ref, row, part, group):
        return ref[row % RING, part * SUBLANES : (part + 1) * SUBLANES, group * LANES : (group + 1) * LANES]

    def advance(step, top, base):
        source = states[step - 1]
        weights = [
            jnp.broadcast_to(weight_ref[:, g * LANES : (g + 1) * LANES], (SUBLANES, LANES)) for g in range(groups)
        ]
        block = [(o, g) for g in range(groups) for o in range(BLOCK)]
        start = {(o, g): tile(source, top + o, 0, g) for o, g in block}
        wrapped = {k: pltpu.roll(x, SUBLANES - 1, 0) for k, x in start.items()}
        south = {(o, g): pltpu.roll(tile(source, top + o, per - 1, g), 1, 0) for o, g in block}
        centre = start
        for part in range(per):
            here = slice(part * SUBLANES, (part + 1) * SUBLANES)
            north = wrapped
            if part < per - 1:
                north = {(o, g): tile(source, top + o, part + 1, g) for o, g in block}
            sums = {}
            for o, g in block:
                row = top + o
                west = centre[o - 1, g] if o else tile(source, row - 1, part, g)
                east = centre[o + 1, g] if o < BLOCK - 1 else tile(source, row + 1, part, g)
                c0, ce, cw, cn, cs = (tile(ref, row, part, g) for ref in coefs)
                fresh = (c0 * centre[o, g] + (ce * east + cw * west)) + (cn * north[o, g] + cs * south[o, g])
                if step < STEPS:
                    states[step][row % RING, here, g * LANES : (g + 1) * LANES] = fresh
                else:
                    scaled = fresh * weights[g]
                    both = (scaled, scaled * fresh)
                    sums[o] = tuple(x + y for x, y in zip(sums[o], both)) if o in sums else both
            south, centre = centre, north
            if step == STEPS:
                for which in range(2):
                    kept = out_ref[which, here]
                    for o in range(BLOCK):
                        total = jnp.sum(sums[o][which], axis=1, keepdims=True)
                        kept = jnp.where(column == base + top + o - STEPS, total, kept)
                    out_ref[which, here] = kept

    left_side(0, 0)
    for kind in range(kinds):
        parameter(kind, 0)

    def body(trip, carry):
        base = trip * RING
        for half in range(UNROLL):
            following = (half + 1) % UNROLL
            left_side(base + (half + 1) * BLOCK, following)
            kind = 0
            units = [(s, half * BLOCK - s) for s in range(1, STEPS + 1)]
            for number, (step, row) in enumerate(units):
                advance(step, row, base)
                while kind * len(units) < kinds * (number + 1):
                    parameter(kind, following)
                    kind += 1
        return carry

    lax.fori_loop(0, pl.cdiv(rows, RING), body, 0)


def on_device(field_modes, node_points, quad_weight, group_of):
    kinds, modes, tile_rows, tile_cols = field_modes.shape
    node_count = group_of.shape[0]
    members = lax.axis_size("nodes")
    most = node_count // 2 + node_count // 8
    slots = -(-most // (members * LANES)) * LANES
    member = lax.axis_index("nodes")

    included = group_of < 2
    weight = quad_weight * included.astype(jnp.float32)
    number = jnp.arange(node_count, dtype=jnp.int32)
    before = (number[None, :] < number[:, None]) & included[None, :]
    position = jnp.sum(before.astype(jnp.float32), axis=1).astype(jnp.int32)
    target = jnp.arange(slots, dtype=jnp.int32) * members + member
    select = (included[:, None] & (position[:, None] == target[None, :])).astype(jnp.float32)
    columns = jnp.concatenate([jnp.ones((node_count, 1), jnp.float32), node_points, quad_weight[:, None]], axis=1)
    chosen = lax.dot_general(columns, select, (((0,), (0,)), ((), ())), precision=lax.Precision.HIGHEST)
    slot_coeff, slot_weight = chosen[: modes], chosen[modes:]
    half = 0.5 * TIME_STEP
    mix = (
        ((1.0, 0.0, 0.0, 0.0), 0.0),
        ((0.0, 0.0, 0.0, -4.0 * TIME_STEP), 1.0),
        ((0.0, -half, 0.0, TIME_STEP), 0.0),
        ((0.0, half, 0.0, TIME_STEP), 0.0),
        ((0.0, 0.0, -half, TIME_STEP), 0.0),
        ((0.0, 0.0, half, TIME_STEP), 0.0),
    )
    used = kinds * modes
    padded = -(-(used + 1) // SUBLANES) * SUBLANES
    mixes = jnp.array([m for m, _ in mix], jnp.float32)
    constant = jnp.array([c for _, c in mix], jnp.float32)
    table = (mixes[:, :, None, None] * slot_coeff[None, None]).reshape(len(mix), used, slots)
    table = jnp.concatenate(
        [
            table,
            jnp.broadcast_to(constant[:, None, None], (len(mix), 1, slots)),
            jnp.zeros((len(mix), padded - used - 1, slots), jnp.float32),
        ],
        axis=1,
    )

    def ring(axis):
        size = lax.axis_size(axis)
        up = [(i, (i + 1) % size) for i in range(size)]
        return up, [(j, i) for i, j in up]

    fields = field_modes.reshape(used, tile_rows, tile_cols)
    up, down = ring("gx")
    above = lax.ppermute(fields[:, tile_rows - STEPS :], "gx", up)
    below = lax.ppermute(fields[:, :STEPS], "gx", down)
    tall = jnp.concatenate([above, fields, below], axis=1)
    up, down = ring("gy")


    def columns_of(start):
        parts = [jnp.transpose(x[:, :, start : start + STEPS], (2, 0, 1)) for x in (above, fields, below)]
        return jnp.concatenate(parts, axis=2)

    left = lax.ppermute(columns_of(tile_cols - STEPS), "gy", up)
    right = lax.ppermute(columns_of(0), "gy", down)
    edge = jnp.transpose(jnp.concatenate([left, right], axis=0), (2, 1, 0))
    centre = jnp.transpose(tall, (1, 0, 2))
    fill = ((0, 0), (0, padded - used), (0, 0))
    centre = jnp.pad(centre, fill, constant_values=1.0)
    edge = jnp.pad(edge, fill, constant_values=1.0)

    cells = tile_cols + 2 * STEPS
    per = cells // SUBLANES
    place = jnp.arange(cells, dtype=jnp.int32)
    wanted = (place % SUBLANES) * per + place // SUBLANES - STEPS
    source = jnp.where(
        wanted < 0, tile_cols + STEPS + wanted, jnp.where(wanted < tile_cols, wanted, wanted + STEPS)
    )
    order = (source[:, None] == place[None, :]).astype(jnp.bfloat16)

    sums = pl.pallas_call(
        moments_kernel,
        out_shape=jax.ShapeDtypeStruct((2, cells, tile_rows), jnp.float32),
        scratch_shapes=[
            pltpu.VMEM((len(mix), 3 * padded, slots), jnp.bfloat16),
            pltpu.VMEM((UNROLL, BLOCK * cells, 3 * padded), jnp.bfloat16),
        ]
        + [pltpu.VMEM((RING, cells, slots), jnp.float32)] * (len(mix) + STEPS - 1),
        compiler_params=pltpu.CompilerParams(vmem_limit_bytes=48 * 1024 * 1024),
        name="moments",
    )(centre, edge, table, slot_weight, order)

    total = sums
    for shift in range(1, members):
        ring_pairs = [(i, (i + shift) % members) for i in range(members)]
        total = total + lax.ppermute(sums, "nodes", ring_pairs)
    weight_total = jnp.sum(weight)
    mean = total[0] / weight_total
    variance = total[1] / weight_total - mean * mean
    fields_out = jnp.stack([mean, variance]).reshape(2, per, SUBLANES, tile_rows)
    fields_out = jnp.transpose(fields_out, (0, 3, 2, 1)).reshape(2, tile_rows, cells)
    fields_out = fields_out[:, :, STEPS : STEPS + tile_cols]
    return fields_out[0], fields_out[1]


def solution(mesh):
    placed = (P(None, None, "gx", "gy"), P(), P(), P())
    return jax.shard_map(
        on_device,
        mesh=mesh,
        in_specs=placed,
        out_specs=(P("gx", "gy"), P("gx", "gy")),
        check_vma=False,
    )
```
